32 devices in a mesh: copies: 2 (over y), oct: 4 (over z), leaf: 4 (over x, core).
Axes of the slice: x: 2, y: 2, z: 4, core: 2. Of those that a mesh axis runs over, the one named last changes fastest.
Arguments:
- coords: float32 [3, 65536], P(None, ('copies', 'oct')), parts along dimension 1, may hold values from 0 to 1, as said below
- skeleton: float32 [3, 32, 128], P(None, None, 'copies'), parts along dimension 2, may hold values from 0 to 1, as said below
- basis: bfloat16 [32, 65536], P(None, ('copies', 'oct', 'leaf')), parts along dimension 1, may hold values from -1.5 to 1.5
- probes: bfloat16 [65536, 128], P(('copies', 'oct', 'leaf')), parts along dimension 0, may hold values from -6 to 6
- near_list: int32 [128, 27], P(('copies', 'oct', 'leaf')), parts along dimension 0, may hold values from 0 to 63, as said below
- far_list: int32 [128, 32], P('copies'), parts along dimension 0, may hold values from 0 to 63, as said below
Outputs:
- product: bfloat16 [65536, 128], P(('copies', 'oct', 'leaf')), parts along dimension 0
The draws below stay inside these ranges and needn't reach their ends.
There are 2 independent parts, one for each index of `copies`. The reference program is written for one: setup_inputs(seed, part) draws one part's arguments, and reference() takes and returns one part's arrays. A program takes and returns all parts, laid end to end along the dimension named above; each array names one. Nothing has to cross between parts.
Inputs may be any that keep to these rules, and one draw needn't show every extreme that they name: `coords`: the points of leaf block b lie in b's octree cell, whose corner follows from the bits of b taken in turn for the three components. The skeleton points of leaf block b lie in b's octree cell. `near_list`: entry 0 of row a is a. The other entries name leaf blocks of a's octant group held by a's device d = a // 4 or by the device just before or after it along leaf within the group; entries may repeat. `far_list`: every entry names a leaf block of another octant group than its row's (group = block // 16). Among the rows of one device, the entries that name blocks of any one other device number at most 11, and exactly 11 for some device; entries may repeat.
All inputs are finite; a program needn't handle non-finite values.
Results may differ from the reference program's by a relative error of at most 0.005.
Values may be sent and summed in bfloat16 or wider, within the bound.
A program may use at most 64 MiB of HBM per device.

```python
import math
import jax
import jax.numpy as jnp
from jax import lax

LEAF = 512
RANK = 32
RHS = 128
NEAR = 27
FAR = 32
LEAVES_DEV = 4
LEAVES = 64
POINTS = 32768
N_OCT = 4
N_LEAF = 4


def leaf_cells(leaf_ids):
    bit_count = max((LEAVES - 1).bit_length(), 1)
    cells = []
    sides = []
    for axis_pos in range(3):
        cell = jnp.zeros_like(leaf_ids)
        shift_count = 0
        for bit_pos in range(axis_pos, bit_count, 3):
            cell = cell + jnp.left_shift(jnp.right_shift(leaf_ids, bit_pos) & 1, shift_count)
            shift_count = shift_count + 1
        cells.append(cell)
        sides.append(float(2 ** shift_count))
    return (cells, sides)


def draw_coords(key, part):
    leaf_ids = jnp.arange(LEAVES, dtype=jnp.int32)
    cells, sides = leaf_cells(leaf_ids)
    jitter = jax.random.uniform(key, (3, LEAVES, LEAF), jnp.float32)
    stacked = jnp.stack([(cells[pos][:, None].astype(jnp.float32) + jitter[pos]) / sides[pos] for pos in range(3)])
    return stacked.reshape(3, POINTS).astype(jnp.float32)


def draw_skeleton(key, part):
    leaf_ids = jnp.arange(LEAVES, dtype=jnp.int32)
    cells, sides = leaf_cells(leaf_ids)
    jitter = jax.random.uniform(jax.random.fold_in(key, 7), (3, RANK, LEAVES), jnp.float32)
    stacked = jnp.stack([(cells[pos][None, :].astype(jnp.float32) + jitter[pos]) / sides[pos] for pos in range(3)])
    return stacked.astype(jnp.float32)


def draw_near_list(key, part):
    leaf_ids = jnp.arange(LEAVES, dtype=jnp.int32)
    device_ids = leaf_ids // LEAVES_DEV
    group_start = device_ids // N_LEAF * N_LEAF
    lowest = jnp.maximum(device_ids - 1, group_start) * LEAVES_DEV
    highest = (jnp.minimum(device_ids + 1, group_start + N_LEAF - 1) + 1) * LEAVES_DEV
    picks = jax.random.randint(jax.random.fold_in(key, 11), (LEAVES, NEAR - 1), lowest[:, None], highest[:, None])
    return jnp.concatenate([leaf_ids[:, None], picks.astype(jnp.int32)], axis=1)


def draw_far_list(key, part):
    others = N_LEAF * (N_OCT - 1)
    requests = LEAVES_DEV * FAR
    slots = (requests + others - 1) // others
    device_total = N_OCT * N_LEAF

    def one_device(device_id, device_key):
        keys = jax.random.split(device_key, slots + 2)
        order = jnp.concatenate([jax.random.permutation(keys[pos], others) for pos in range(slots)])[:requests]
        order = jax.random.permutation(keys[slots], order)
        own_group = device_id // N_LEAF
        target_group = order // N_LEAF
        target_group = target_group + (target_group >= own_group).astype(jnp.int32)
        owner = target_group * N_LEAF + order % N_LEAF
        local = jax.random.randint(keys[slots + 1], (requests,), 0, LEAVES_DEV)
        return (owner * LEAVES_DEV + local).astype(jnp.int32).reshape(LEAVES_DEV, FAR)
    device_keys = jax.random.split(jax.random.fold_in(key, 13), device_total)
    table = jax.vmap(one_device)(jnp.arange(device_total, dtype=jnp.int32), device_keys)
    return table.reshape(LEAVES, FAR).astype(jnp.int32)


def block_levels(own_key, dims, pieces, low, top_value):
    def one(axis_at, parts):
        draws = jax.random.uniform(jax.random.fold_in(jax.random.fold_in(own_key, 6), axis_at), (parts,), jnp.float32, low / len(pieces), top_value / len(pieces))
        return jnp.repeat(jnp.exp(draws), dims[axis_at] // parts).reshape((-1,) + (1,) * (len(dims) - axis_at - 1))

    factor_of = one(*pieces[0])
    for cut in pieces[1:]:
        factor_of = factor_of * one(*cut)
    return factor_of


def noise(key, extent, deviation, reach, cuts=(), held_as=jnp.bfloat16):
    array = jax.random.normal(key, extent, jnp.float32) * deviation
    if len(cuts) > 0:
        array = block_levels(key, extent, cuts, -0.22, 0.18) * array
    return jnp.clip(array, min=-reach, max=reach).astype(held_as)


def setup_inputs(seed: int = 0, part: int = 0) -> dict:
    key_of = jax.random.split(jax.random.key(seed), 7)
    own_keys = jax.random.split(jax.random.fold_in(key_of[6], part), 7)
    coords = draw_coords(jax.random.fold_in(jax.random.fold_in(key_of[6], part), 71), part)
    skeleton = draw_skeleton(jax.random.fold_in(jax.random.fold_in(key_of[6], part), 71), part)
    basis = noise(own_keys[2], (RANK, POINTS), (LEAF // RANK) ** -0.5, 1.5, ((1, 16),))
    probes = noise(own_keys[3], (POINTS, RHS), 1.0, 6.0, ((0, 16),))
    near_list = draw_near_list(jax.random.fold_in(jax.random.fold_in(key_of[6], part), 71), part)
    far_list = draw_far_list(jax.random.fold_in(jax.random.fold_in(key_of[6], part), 71), part)
    return {"coords": coords, "skeleton": skeleton, "basis": basis, "probes": probes, "near_list": near_list, "far_list": far_list}


length_scale = 0.4
root_three = math.sqrt(3.0)

def matern(dist_sq):
    scaled = jnp.sqrt(dist_sq) * (root_three / length_scale)
    return (1.0 + scaled) * jnp.exp(-scaled)

def reference(coords, skeleton, basis, probes, near_list, far_list):
    scale = 1.0 / math.sqrt(NEAR * LEAF)
    coords_leaf = coords.reshape(3, LEAVES, LEAF)
    probe_leaf = probes.reshape(LEAVES, LEAF, RHS)
    basis_leaf = basis.reshape(RANK, LEAVES, LEAF)
    coef = jnp.einsum('mal,alh->amh', basis_leaf.astype(jnp.float32), probe_leaf.astype(jnp.float32)).astype(jnp.bfloat16)

    def one_leaf(leaf_pos):
        own_points = lax.dynamic_index_in_dim(coords_leaf, leaf_pos, 1, keepdims=False)
        near_ids = lax.dynamic_index_in_dim(near_list, leaf_pos, 0, keepdims=False).astype(jnp.int32)
        near_points = jnp.take(coords_leaf, near_ids, axis=1)
        dist_sq = jnp.square(own_points[0][None, :, None] - near_points[0][:, None, :])
        dist_sq = dist_sq + jnp.square(own_points[1][None, :, None] - near_points[1][:, None, :])
        dist_sq = dist_sq + jnp.square(own_points[2][None, :, None] - near_points[2][:, None, :])
        panel = matern(dist_sq).astype(jnp.bfloat16)
        near_rows = jnp.take(probe_leaf, near_ids, axis=0)
        near_sum = jnp.einsum('kij,kjh->ih', panel.astype(jnp.float32), near_rows.astype(jnp.float32))
        far_ids = lax.dynamic_index_in_dim(far_list, leaf_pos, 0, keepdims=False).astype(jnp.int32)
        own_skel = lax.dynamic_index_in_dim(skeleton, leaf_pos, 2, keepdims=False)
        far_skel = jnp.take(skeleton, far_ids, axis=2)
        skel_sq = jnp.square(own_skel[0][None, :, None] - jnp.transpose(far_skel[0])[:, None, :])
        skel_sq = skel_sq + jnp.square(own_skel[1][None, :, None] - jnp.transpose(far_skel[1])[:, None, :])
        skel_sq = skel_sq + jnp.square(own_skel[2][None, :, None] - jnp.transpose(far_skel[2])[:, None, :])
        coupling = matern(skel_sq).astype(jnp.bfloat16)
        picked = jnp.take(coef, far_ids, axis=0)
        far_coef = jnp.einsum('kmn,knh->mh', coupling.astype(jnp.float32), picked.astype(jnp.float32)).astype(jnp.bfloat16)
        own_basis = lax.dynamic_index_in_dim(basis_leaf, leaf_pos, 1, keepdims=False)
        far_sum = jnp.einsum('ml,mh->lh', own_basis.astype(jnp.float32), far_coef.astype(jnp.float32))
        return ((near_sum + far_sum) * scale).astype(jnp.bfloat16)
    blocks = lax.map(one_leaf, jnp.arange(LEAVES, dtype=jnp.int32))
    return blocks.reshape(POINTS, RHS)
```

```python
import functools
import math

import jax
import jax.numpy as jnp
from jax import lax
from jax.experimental import pallas as pl
from jax.experimental.pallas import tpu as pltpu
from jax.sharding import PartitionSpec as P

LEAF = 512
RANK = 32
RHS = 128
NEAR = 27
FAR = 32

LN2 = math.log(2.0)
UNIT = math.sqrt(3.0) / 0.4 / LN2
TINY = 1e-24
FEATURES = 64
MESH = pl.DeviceIdType.MESH
F32 = jnp.float32
BF16 = jnp.bfloat16


def split(x):
    first = x.astype(BF16).astype(F32)
    second = (x - first).astype(BF16).astype(F32)
    return first, second, x - first - second


def features(x, left):
    x1, x2, x3 = split(x)
    n1, n2, n3 = split(jnp.sum(x * x, axis=0, keepdims=True))
    row = lax.broadcasted_iota(jnp.int32, x.shape, 0)
    norm = jnp.where(row == 0, n1, jnp.where(row == 1, n2, jnp.where(row == 2, n3, 0.0)))
    ones = jnp.where(row < 3, 1.0, 0.0)
    if left:
        y1, y2, y3 = -2.0 * x1, -2.0 * x2, -2.0 * x3
        return jnp.concatenate([y1, y1, y2, y2, y1, y3, ones, norm], axis=0)
    return jnp.concatenate([x1, x2, x1, x2, x3, x1, norm, ones], axis=0)


def weighted(dist, weight):
    x = jnp.maximum(dist, TINY)
    s = x * lax.rsqrt(x)
    return ((weight + (weight * LN2) * s) * jnp.exp2(-s)).astype(BF16)


def kernel(
    n_oct, n_leaf, per_dev,
    coords_ref, skel_ref, basis_ref, probes_ref, near_ref, far_ref, out_ref,
    pts, skel, own_feat, acc, window, coefs, weights,
    near_send, near_recv, oct_send, oct_recv, leaf_send, leaf_recv,
):
    me_oct = lax.axis_index("oct")
    me = lax.axis_index("leaf")
    me_copy = lax.axis_index("copies")
    rows = per_dev * LEAF
    ranks = per_dev * RANK
    partner = me + 1 - 2 * lax.rem(me, 2)
    other = me - 1 + 2 * lax.rem(me, 2)
    sides = (partner, other)
    exists = [jnp.logical_and(side >= 0, side < n_leaf) for side in sides]

    def at(o, l):
        return (me_copy, o, l)

    barrier = pltpu.get_barrier_semaphore()
    for k in range(1, n_oct):
        pl.semaphore_signal(
            barrier, inc=1, device_id=at(lax.rem(me_oct + k, n_oct), me), device_id_type=MESH
        )
    for k in range(1, n_leaf):
        pl.semaphore_signal(
            barrier, inc=1, device_id=at(me_oct, lax.rem(me + k, n_leaf)), device_id_type=MESH
        )

    for j in range(per_dev):
        own = jnp.dot(
            basis_ref[:, j * LEAF:(j + 1) * LEAF],
            probes_ref[j * LEAF:(j + 1) * LEAF, :],
            preferred_element_type=F32,
        )
        coefs[me_oct, me, j * RANK:(j + 1) * RANK, :] = own.astype(BF16)

    pl.semaphore_wait(barrier, n_oct + n_leaf - 2)

    def near_copy(slot):
        return pltpu.make_async_remote_copy(
            src_ref=probes_ref, dst_ref=window.at[slot],
            send_sem=near_send.at[slot], recv_sem=near_recv.at[slot],
            device_id=at(me_oct, sides[slot]), device_id_type=MESH,
        )

    for slot in range(2):
        @pl.when(exists[slot])
        def _():
            near_copy(slot).start()

    pts[...] = jnp.zeros_like(pts)
    pts[0:3, :] = (coords_ref[...] - 0.5) * UNIT
    skel[...] = jnp.zeros_like(skel)
    skel[0:3, :] = (skel_ref[...] - 0.5) * UNIT
    own_x = pts[:, pl.ds(pl.multiple_of(me * rows, rows), rows)]
    own_feat[...] = features(own_x, False).astype(BF16)
    acc[...] = jnp.zeros_like(acc)
    near = near_ref[...]

    oct_copies = []
    for k in range(1, n_oct):
        oct_copies.append(pltpu.make_async_remote_copy(
            src_ref=coefs.at[me_oct, me], dst_ref=coefs.at[me_oct, me],
            send_sem=oct_send.at[k - 1], recv_sem=oct_recv.at[k - 1],
            device_id=at(lax.rem(me_oct + k, n_oct), me), device_id_type=MESH,
        ))
    for copy in oct_copies:
        copy.start()

    def near_block(source, read):
        first = (me_oct * n_leaf + source) * per_dev

        def body(c, carry):
            x = pts[:, pl.ds(pl.multiple_of(source * rows + c * LEAF, LEAF), LEAF)]
            left = features(x, True).T.astype(BF16)
            count = jnp.sum(
                jnp.where(near == first + c, 1.0, 0.0), axis=1, keepdims=True
            )
            weights[0:per_dev, :] = jnp.broadcast_to(count, (per_dev, LEAF))
            side = read(c).astype(F32).T.astype(BF16)
            for a in range(per_dev):
                cols = slice(a * LEAF, (a + 1) * LEAF)
                dist = jnp.dot(left, own_feat[:, cols], preferred_element_type=F32)
                panel = weighted(dist, weights[a:a + 1, :])
                acc[:, cols] += jnp.dot(side, panel, preferred_element_type=F32)
            return carry

        lax.fori_loop(0, per_dev, body, 0)

    near_block(me, lambda c: probes_ref[pl.ds(pl.multiple_of(c * LEAF, LEAF), LEAF), :])

    for copy in oct_copies:
        copy.wait()
    leaf_copies = []
    for k in range(1, n_leaf):
        leaf_copies.append(pltpu.make_async_remote_copy(
            src_ref=coefs.at[:, me], dst_ref=coefs.at[:, me],
            send_sem=leaf_send.at[k - 1], recv_sem=leaf_recv.at[k - 1],
            device_id=at(me_oct, lax.rem(me + k, n_leaf)), device_id_type=MESH,
        ))
    for copy in leaf_copies:
        copy.start()

    for slot in range(2):
        @pl.when(exists[slot])
        def _():
            near_copy(slot).wait()
            near_block(
                sides[slot],
                lambda c: window[slot, pl.ds(pl.multiple_of(c * LEAF, LEAF), LEAF), :],
            )

    for copy in leaf_copies:
        copy.wait()

    dev = me_oct * n_leaf + me
    mine = skel[:, pl.ds(pl.multiple_of(dev * ranks, ranks), ranks)]
    left = features(mine, True).T.astype(BF16)
    far = far_ref[...]
    far_coef = jnp.zeros((ranks, RHS), F32)
    for o in range(n_oct):
        width = n_leaf * ranks
        right = features(skel[:, o * width:(o + 1) * width], False).astype(BF16)
        dist = jnp.dot(left, right, preferred_element_type=F32)
        leaf_id = lax.broadcasted_iota(jnp.int32, (per_dev, width), 1) // RANK + o * n_leaf * per_dev
        count = jnp.zeros((per_dev, width), F32)
        for j in range(FAR):
            count += jnp.where(far[:, j:j + 1] == leaf_id, 1.0, 0.0)
        weight = jnp.concatenate(
            [jnp.broadcast_to(count[a:a + 1, :], (RANK, width)) for a in range(per_dev)], axis=0
        )
        block = coefs[o].reshape(width, RHS)
        far_coef += jnp.dot(weighted(dist, weight), block, preferred_element_type=F32)
    far_side = far_coef.T.astype(BF16)
    scale = 1.0 / math.sqrt(NEAR * LEAF)
    owner = lax.broadcasted_iota(jnp.int32, (ranks, LEAF), 0) // RANK
    for a in range(per_dev):
        cols = slice(a * LEAF, (a + 1) * LEAF)
        tiled = jnp.concatenate([basis_ref[:, cols].astype(F32)] * per_dev, axis=0)
        block = jnp.where(owner == a, tiled, 0.0).astype(BF16)
        total = acc[:, cols] + jnp.dot(far_side, block, preferred_element_type=F32)
        out_ref[cols, :] = (total * scale).T.astype(BF16)


def local(coords, skeleton, basis, probes, near_list, far_list):
    per_dev = near_list.shape[0]
    n_leaf = lax.axis_size("leaf")
    n_oct = lax.axis_size("oct")
    rows = per_dev * LEAF
    ranks = per_dev * RANK
    leaves = n_oct * n_leaf * per_dev
    dev = lax.axis_index(("oct", "leaf"))
    own_far = lax.dynamic_slice_in_dim(far_list, dev * per_dev, per_dev, 0)
    skel = jnp.transpose(skeleton, (0, 2, 1)).reshape(3, leaves * RANK)
    vmem = pl.BlockSpec(memory_space=pltpu.VMEM)
    return pl.pallas_call(
        functools.partial(kernel, n_oct, n_leaf, per_dev),
        out_shape=jax.ShapeDtypeStruct((rows, RHS), BF16),
        in_specs=[vmem] * 6,
        out_specs=vmem,
        scratch_shapes=[
            pltpu.VMEM((8, n_leaf * rows), F32),
            pltpu.VMEM((8, leaves * RANK), F32),
            pltpu.VMEM((FEATURES, rows), BF16),
            pltpu.VMEM((RHS, rows), F32),
            pltpu.VMEM((2, rows, RHS), BF16),
            pltpu.VMEM((n_oct, n_leaf, ranks, RHS), BF16),
            pltpu.VMEM((8, LEAF), F32),
            pltpu.SemaphoreType.DMA((2,)),
            pltpu.SemaphoreType.DMA((2,)),
            pltpu.SemaphoreType.DMA((n_oct - 1,)),
            pltpu.SemaphoreType.DMA((n_oct - 1,)),
            pltpu.SemaphoreType.DMA((n_leaf - 1,)),
            pltpu.SemaphoreType.DMA((n_leaf - 1,)),
        ],
        compiler_params=pltpu.CompilerParams(
            collective_id=0, has_side_effects=True, vmem_limit_bytes=60 * 1024 * 1024
        ),
    )(coords, skel, basis, probes, near_list, own_far)


def solution(mesh):
    in_specs = (
        P(None, ("copies", "oct")),
        P(None, None, "copies"),
        P(None, ("copies", "oct", "leaf")),
        P(("copies", "oct", "leaf"), None),
        P(("copies", "oct", "leaf"), None),
        P("copies", None),
    )
    out_specs = P(("copies", "oct", "leaf"), None)
    return jax.shard_map(local, mesh=mesh, in_specs=in_specs, out_specs=out_specs, check_vma=False)
```

```python
import functools
import math

import jax
import jax.numpy as jnp
from jax import lax
from jax.experimental import pallas as pl
from jax.experimental.pallas import tpu as pltpu
from jax.sharding import PartitionSpec as P

LEAF = 512
RANK = 32
RHS = 128
NEAR = 27
FAR = 32

LN2 = math.log(2.0)
UNIT = math.sqrt(3.0) / 0.4
TINY = 1e-24
FEATURES = 64
MESH = pl.DeviceIdType.MESH
F32 = jnp.float32
BF16 = jnp.bfloat16


def split(x):
    first = x.astype(BF16).astype(F32)
    second = (x - first).astype(BF16).astype(F32)
    return first, second, x - first - second


def features(x, left):
    x1, x2, x3 = split(x)
    n1, n2, n3 = split(jnp.sum(x * x, axis=0, keepdims=True))
    row = lax.broadcasted_iota(jnp.int32, x.shape, 0)
    norm = jnp.where(row == 0, n1, jnp.where(row == 1, n2, jnp.where(row == 2, n3, 0.0)))
    ones = jnp.where(row < 3, 1.0, 0.0)
    if left:
        y1, y2, y3 = -2.0 * x1, -2.0 * x2, -2.0 * x3
        return jnp.concatenate([y1, y1, y2, y2, y1, y3, ones, norm], axis=0)
    return jnp.concatenate([x1, x2, x1, x2, x3, x1, norm, ones], axis=0)


def matern(dist):
    x = jnp.maximum(dist, TINY)
    t = x * lax.rsqrt(x)
    return (1.0 + t) * jnp.exp2(t * (-1.0 / LN2))


def kernel(
    n_oct, n_leaf, per_dev,
    coords_ref, skel_ref, basis_ref, probes_ref, near_ref, far_ref, out_ref,
    pts, skel, own_feat, acc, window, coefs, weights,
    dist_even, dist_odd, panel_even, panel_odd, side_even, side_odd, left_even, left_odd,
    near_send, near_recv, oct_send, oct_recv, leaf_send, leaf_recv,
):
    me_oct = lax.axis_index("oct")
    me = lax.axis_index("leaf")
    me_copy = lax.axis_index("copies")
    rows = per_dev * LEAF
    ranks = per_dev * RANK
    partner = me + 1 - 2 * lax.rem(me, 2)
    other = me - 1 + 2 * lax.rem(me, 2)
    sides = (partner, other)
    exists = [jnp.logical_and(side >= 0, side < n_leaf) for side in sides]

    def at(o, l):
        return (me_copy, o, l)

    barrier = pltpu.get_barrier_semaphore()
    for k in range(1, n_oct):
        pl.semaphore_signal(
            barrier, inc=1, device_id=at(lax.rem(me_oct + k, n_oct), me), device_id_type=MESH
        )
    for k in range(1, n_leaf):
        pl.semaphore_signal(
            barrier, inc=1, device_id=at(me_oct, lax.rem(me + k, n_leaf)), device_id_type=MESH
        )

    for j in range(per_dev):
        own = jnp.dot(
            basis_ref[:, j * LEAF:(j + 1) * LEAF],
            probes_ref[j * LEAF:(j + 1) * LEAF, :],
            preferred_element_type=F32,
        )
        coefs[me_oct, me, j * RANK:(j + 1) * RANK, :] = own.astype(BF16)

    pl.semaphore_wait(barrier, n_oct + n_leaf - 2)

    def near_copy(slot):
        return pltpu.make_async_remote_copy(
            src_ref=probes_ref, dst_ref=window.at[slot + 1],
            send_sem=near_send.at[slot], recv_sem=near_recv.at[slot],
            device_id=at(me_oct, sides[slot]), device_id_type=MESH,
        )

    near_copy(0).start()

    @pl.when(exists[1])
    def _():
        near_copy(1).start()

    pts[...] = jnp.zeros_like(pts)
    pts[0:3, :] = (coords_ref[...] - 0.5) * UNIT
    skel[...] = jnp.zeros_like(skel)
    skel[0:3, :] = (skel_ref[...] - 0.5) * UNIT
    own_x = pts[:, pl.ds(pl.multiple_of(me * rows, rows), rows)]
    own_feat[...] = features(own_x, False).astype(BF16)
    acc[...] = jnp.zeros_like(acc)
    near = near_ref[...]

    oct_copies = []
    for k in range(1, n_oct):
        oct_copies.append(pltpu.make_async_remote_copy(
            src_ref=coefs.at[me_oct, me], dst_ref=coefs.at[me_oct, me],
            send_sem=oct_send.at[k - 1], recv_sem=oct_recv.at[k - 1],
            device_id=at(lax.rem(me_oct + k, n_oct), me), device_id_type=MESH,
        ))
    for copy in oct_copies:
        copy.start()

    leaf_copies = []
    for k in range(1, n_leaf):
        leaf_copies.append(pltpu.make_async_remote_copy(
            src_ref=coefs.at[:, me], dst_ref=coefs.at[:, me],
            send_sem=leaf_send.at[k - 1], recv_sem=leaf_recv.at[k - 1],
            device_id=at(me_oct, lax.rem(me + k, n_leaf)), device_id_type=MESH,
        ))

    dists, panels = (dist_even, dist_odd), (panel_even, panel_odd)
    lefts, side_refs = (left_even, left_odd), (side_even, side_odd)
    total = (2 + exists[1].astype(jnp.int32)) * per_dev

    def source_of(g):
        slot = g // per_dev
        return jnp.where(slot == 0, me, jnp.where(slot == 1, partner, other))

    def fill_left(g, ref):
        g = jnp.minimum(g, total - 1)
        start = source_of(g) * rows + lax.rem(g, per_dev) * LEAF
        ref[...] = features(pts[:, pl.ds(pl.multiple_of(start, LEAF), LEAF)], True).T.astype(BF16)

    def fill_side(g, ref):
        start = pl.multiple_of(lax.rem(g, per_dev) * LEAF, LEAF)
        ref[...] = window[g // per_dev, pl.ds(start, LEAF), :].astype(F32).T.astype(BF16)

    def fill_dist(half, ref, left, a):
        part = slice(half * LEAF // 2, (half + 1) * LEAF // 2)
        ref[part, :] = jnp.dot(
            left[part, :], own_feat[:, a * LEAF:(a + 1) * LEAF], preferred_element_type=F32
        )

    def fill_panel(part, ref, dist):
        for r in range(part * LEAF // 8, (part + 1) * LEAF // 8, 16):
            ref[r:r + 16, :] = matern(dist[r:r + 16, :]).astype(BF16)

    def apply(half, g, a, side, panel):
        width = LEAF // 2
        cols = slice(a * LEAF + half * width, a * LEAF + (half + 1) * width)
        got = jnp.dot(
            side[...], panel[:, half * width:(half + 1) * width], preferred_element_type=F32
        )
        acc[:, cols] += got * weights[g, a:a + 1, :width]

    for g in range(3 * per_dev):
        first = (me_oct * n_leaf + source_of(g)) * per_dev + g % per_dev
        count = jnp.sum(jnp.where(near == first, 1.0, 0.0), axis=1, keepdims=True)
        weights[g, 0:per_dev, :] = jnp.broadcast_to(count, (per_dev, LEAF // 2))
    window[0] = probes_ref[...]
    side_odd[...] = jnp.zeros_like(side_odd)
    panel_odd[...] = jnp.zeros_like(panel_odd)
    fill_left(0, left_even)
    for half in range(2):
        fill_dist(half, dist_even, left_even, 0)

    steps = 2 * per_dev

    def body(pair, carry):
        g = pair * 2

        @pl.when(g == per_dev)
        def _():
            near_copy(0).wait()
            for copy in oct_copies:
                copy.wait()
            for copy in leaf_copies:
                copy.start()

        @pl.when(g == 2 * per_dev)
        def _():
            near_copy(1).wait()

        for i in range(steps):
            later = (i + 1) % steps
            before = (i - 1) % steps
            before_g = jnp.maximum(g - 1, 0) if i == 0 else g + before // per_dev
            for part in range(8):
                if part == 0 or part == 4:
                    fill_dist(
                        part // 4, dists[later % 2], lefts[later // per_dev], later % per_dev
                    )
                if part == 1 or part == 5:
                    apply(
                        part // 4, before_g, before % per_dev,
                        side_refs[before // per_dev], panels[before % 2],
                    )
                if part == 6 and i == 0:
                    fill_side(g, side_even)
                    fill_left(g + 1, left_odd)
                if part == 6 and i == per_dev:
                    fill_side(g + 1, side_odd)
                    fill_left(g + 2, left_even)
                fill_panel(part, panels[i % 2], dists[i % 2])
        return carry

    lax.fori_loop(0, total // 2, body, 0)
    for half in range(2):
        apply(half, total - 1, per_dev - 1, side_odd, panel_odd)

    for copy in leaf_copies:
        copy.wait()

    dev = me_oct * n_leaf + me
    mine = skel[:, pl.ds(pl.multiple_of(dev * ranks, ranks), ranks)]
    left = features(mine, True).T.astype(BF16)
    far = far_ref[...]
    far_coef = jnp.zeros((ranks, RHS), F32)
    for o in range(n_oct):
        width = n_leaf * ranks
        right = features(skel[:, o * width:(o + 1) * width], False).astype(BF16)
        dist = jnp.dot(left, right, preferred_element_type=F32)
        leaf_id = lax.broadcasted_iota(jnp.int32, (per_dev, width), 1) // RANK + o * n_leaf * per_dev
        count = jnp.zeros((per_dev, width), F32)
        for j in range(FAR):
            count += jnp.where(far[:, j:j + 1] == leaf_id, 1.0, 0.0)
        weight = jnp.concatenate(
            [jnp.broadcast_to(count[a:a + 1, :], (RANK, width)) for a in range(per_dev)], axis=0
        )
        block = coefs[o].reshape(width, RHS)
        far_coef += jnp.dot((matern(dist) * weight).astype(BF16), block, preferred_element_type=F32)
    far_side = far_coef.T.astype(BF16)
    scale = 1.0 / math.sqrt(NEAR * LEAF)
    owner = lax.broadcasted_iota(jnp.int32, (ranks, LEAF), 0) // RANK
    for a in range(per_dev):
        cols = slice(a * LEAF, (a + 1) * LEAF)
        tiled = jnp.concatenate([basis_ref[:, cols].astype(F32)] * per_dev, axis=0)
        block = jnp.where(owner == a, tiled, 0.0).astype(BF16)
        total = acc[:, cols] + jnp.dot(far_side, block, preferred_element_type=F32)
        out_ref[cols, :] = (total * scale).T.astype(BF16)


def local(coords, skeleton, basis, probes, near_list, far_list):
    per_dev = near_list.shape[0]
    n_leaf = lax.axis_size("leaf")
    n_oct = lax.axis_size("oct")
    rows = per_dev * LEAF
    ranks = per_dev * RANK
    leaves = n_oct * n_leaf * per_dev
    dev = lax.axis_index(("oct", "leaf"))
    own_far = lax.dynamic_slice_in_dim(far_list, dev * per_dev, per_dev, 0)
    skel = jnp.transpose(skeleton, (0, 2, 1)).reshape(3, leaves * RANK)
    vmem = pl.BlockSpec(memory_space=pltpu.VMEM)
    return pl.pallas_call(
        functools.partial(kernel, n_oct, n_leaf, per_dev),
        out_shape=jax.ShapeDtypeStruct((rows, RHS), BF16),
        in_specs=[vmem] * 6,
        out_specs=vmem,
        scratch_shapes=[
            pltpu.VMEM((8, n_leaf * rows), F32),
            pltpu.VMEM((8, leaves * RANK), F32),
            pltpu.VMEM((FEATURES, rows), BF16),
            pltpu.VMEM((RHS, rows), F32),
            pltpu.VMEM((3, rows, RHS), BF16),
            pltpu.VMEM((n_oct, n_leaf, ranks, RHS), BF16),
            pltpu.VMEM((3 * per_dev, 8, LEAF // 2), F32),
            pltpu.VMEM((LEAF, LEAF), F32),
            pltpu.VMEM((LEAF, LEAF), F32),
            pltpu.VMEM((LEAF, LEAF), BF16),
            pltpu.VMEM((LEAF, LEAF), BF16),
            pltpu.VMEM((RHS, LEAF), BF16),
            pltpu.VMEM((RHS, LEAF), BF16),
            pltpu.VMEM((LEAF, FEATURES), BF16),
            pltpu.VMEM((LEAF, FEATURES), BF16),
            pltpu.SemaphoreType.DMA((2,)),
            pltpu.SemaphoreType.DMA((2,)),
            pltpu.SemaphoreType.DMA((n_oct - 1,)),
            pltpu.SemaphoreType.DMA((n_oct - 1,)),
            pltpu.SemaphoreType.DMA((n_leaf - 1,)),
            pltpu.SemaphoreType.DMA((n_leaf - 1,)),
        ],
        compiler_params=pltpu.CompilerParams(
            collective_id=0, has_side_effects=True, vmem_limit_bytes=60 * 1024 * 1024
        ),
    )(coords, skel, basis, probes, near_list, own_far)


def solution(mesh):
    in_specs = (
        P(None, ("copies", "oct")),
        P(None, None, "copies"),
        P(None, ("copies", "oct", "leaf")),
        P(("copies", "oct", "leaf"), None),
        P(("copies", "oct", "leaf"), None),
        P("copies", None),
    )
    out_specs = P(("copies", "oct", "leaf"), None)
    return jax.shard_map(local, mesh=mesh, in_specs=in_specs, out_specs=out_specs, check_vma=False)
```

```python
import functools
import math

import jax
import jax.numpy as jnp
from jax import lax
from jax.experimental import pallas as pl
from jax.experimental.pallas import tpu as pltpu
from jax.sharding import PartitionSpec as P

LEAF = 512
RANK = 32
RHS = 128
NEAR = 27
FAR = 32

LN2 = math.log(2.0)
UNIT = math.sqrt(3.0) / 0.4
TINY = 1e-24
FEATURES = 64
MESH = pl.DeviceIdType.MESH
F32 = jnp.float32
BF16 = jnp.bfloat16


def split(x):
    first = x.astype(BF16).astype(F32)
    second = (x - first).astype(BF16).astype(F32)
    return first, second, x - first - second


def features(x, left):
    x1, x2, x3 = split(x)
    n1, n2, n3 = split(jnp.sum(x * x, axis=0, keepdims=True))
    row = lax.broadcasted_iota(jnp.int32, x.shape, 0)
    norm = jnp.where(row == 0, n1, jnp.where(row == 1, n2, jnp.where(row == 2, n3, 0.0)))
    ones = jnp.where(row < 3, 1.0, 0.0)
    if left:
        y1, y2, y3 = -2.0 * x1, -2.0 * x2, -2.0 * x3
        return jnp.concatenate([y1, y1, y2, y2, y1, y3, ones, norm], axis=0)
    return jnp.concatenate([x1, x2, x1, x2, x3, x1, norm, ones], axis=0)


def matern(dist):
    x = jnp.maximum(dist, TINY)
    t = x * lax.rsqrt(x)
    return (1.0 + t) * jnp.exp2(t * (-1.0 / LN2))


def kernel(
    n_oct, n_leaf, per_dev,
    coords_hbm, skel_hbm, basis_hbm, probes_hbm, near_hbm, far_hbm, out_ref,
    pts, skel, own_feat, acc, window, coefs, weights,
    dist_even, dist_odd, panel_even, panel_odd, side_even, side_odd, left_even, left_odd,
    coords_ref, skel_ref, basis_ref, near_ref, far_ref, fetch_sem,
    near_send, near_recv, oct_send, oct_recv, leaf_send, leaf_recv,
):
    me_oct = lax.axis_index("oct")
    me = lax.axis_index("leaf")
    me_copy = lax.axis_index("copies")
    rows = per_dev * LEAF
    ranks = per_dev * RANK
    partner = me + 1 - 2 * lax.rem(me, 2)
    other = me - 1 + 2 * lax.rem(me, 2)
    sides = (partner, other)
    exists = [jnp.logical_and(side >= 0, side < n_leaf) for side in sides]

    def at(o, l):
        return (me_copy, o, l)

    probes_ref = window.at[0]
    fetches = [
        pltpu.make_async_copy(source, target, fetch_sem.at[n])
        for n, (source, target) in enumerate((
            (probes_hbm, probes_ref), (basis_hbm, basis_ref), (coords_hbm, coords_ref),
            (near_hbm, near_ref), (skel_hbm, skel_ref), (far_hbm, far_ref),
        ))
    ]
    for fetch in fetches:
        fetch.start()

    barrier = pltpu.get_barrier_semaphore()
    for k in range(1, n_oct):
        pl.semaphore_signal(
            barrier, inc=1, device_id=at(lax.rem(me_oct + k, n_oct), me), device_id_type=MESH
        )
    for k in range(1, n_leaf):
        pl.semaphore_signal(
            barrier, inc=1, device_id=at(me_oct, lax.rem(me + k, n_leaf)), device_id_type=MESH
        )

    fetches[0].wait()
    fetches[1].wait()
    for j in range(per_dev):
        own = jnp.dot(
            basis_ref[:, j * LEAF:(j + 1) * LEAF],
            probes_ref[j * LEAF:(j + 1) * LEAF, :],
            preferred_element_type=F32,
        )
        coefs[me_oct, me, j * RANK:(j + 1) * RANK, :] = own.astype(BF16)

    pl.semaphore_wait(barrier, n_oct + n_leaf - 2)

    def near_copy(slot):
        return pltpu.make_async_remote_copy(
            src_ref=probes_hbm, dst_ref=window.at[slot + 1],
            send_sem=near_send.at[slot], recv_sem=near_recv.at[slot],
            device_id=at(me_oct, sides[slot]), device_id_type=MESH,
        )

    near_copy(0).start()

    @pl.when(exists[1])
    def _():
        near_copy(1).start()

    for fetch in fetches[2:]:
        fetch.wait()
    pts[...] = jnp.zeros_like(pts)
    pts[0:3, :] = (coords_ref[...] - 0.5) * UNIT
    skel[...] = jnp.zeros_like(skel)
    skel[0:3, :] = (skel_ref[...] - 0.5) * UNIT
    own_x = pts[:, pl.ds(pl.multiple_of(me * rows, rows), rows)]
    own_feat[...] = features(own_x, False).astype(BF16)
    acc[...] = jnp.zeros_like(acc)
    near = near_ref[...]

    oct_copies = []
    for k in range(1, n_oct):
        oct_copies.append(pltpu.make_async_remote_copy(
            src_ref=coefs.at[me_oct, me], dst_ref=coefs.at[me_oct, me],
            send_sem=oct_send.at[k - 1], recv_sem=oct_recv.at[k - 1],
            device_id=at(lax.rem(me_oct + k, n_oct), me), device_id_type=MESH,
        ))
    for copy in oct_copies:
        copy.start()

    leaf_copies = []
    for k in range(1, n_leaf):
        leaf_copies.append(pltpu.make_async_remote_copy(
            src_ref=coefs.at[:, me], dst_ref=coefs.at[:, me],
            send_sem=leaf_send.at[k - 1], recv_sem=leaf_recv.at[k - 1],
            device_id=at(me_oct, lax.rem(me + k, n_leaf)), device_id_type=MESH,
        ))

    dists, panels = (dist_even, dist_odd), (panel_even, panel_odd)
    lefts, side_refs = (left_even, left_odd), (side_even, side_odd)
    total = (2 + exists[1].astype(jnp.int32)) * per_dev

    def source_of(g):
        slot = g // per_dev
        return jnp.where(slot == 0, me, jnp.where(slot == 1, partner, other))

    def fill_left(g, ref):
        g = jnp.minimum(g, total - 1)
        start = source_of(g) * rows + lax.rem(g, per_dev) * LEAF
        ref[...] = features(pts[:, pl.ds(pl.multiple_of(start, LEAF), LEAF)], True).T.astype(BF16)

    def fill_side(g, ref):
        start = pl.multiple_of(lax.rem(g, per_dev) * LEAF, LEAF)
        ref[...] = window[g // per_dev, pl.ds(start, LEAF), :].astype(F32).T.astype(BF16)

    def fill_dist(half, ref, left, a):
        part = slice(half * LEAF // 2, (half + 1) * LEAF // 2)
        ref[part, :] = jnp.dot(
            left[part, :], own_feat[:, a * LEAF:(a + 1) * LEAF], preferred_element_type=F32
        )

    def fill_panel(part, ref, dist):
        for r in range(part * LEAF // 8, (part + 1) * LEAF // 8, 16):
            ref[r:r + 16, :] = matern(dist[r:r + 16, :]).astype(BF16)

    def apply(half, g, a, side, panel):
        width = LEAF // 2
        cols = slice(a * LEAF + half * width, a * LEAF + (half + 1) * width)
        got = jnp.dot(
            side[...], panel[:, half * width:(half + 1) * width], preferred_element_type=F32
        )
        acc[:, cols] += got * weights[g, a:a + 1, :width]

    for g in range(3 * per_dev):
        first = (me_oct * n_leaf + source_of(g)) * per_dev + g % per_dev
        count = jnp.sum(jnp.where(near == first, 1.0, 0.0), axis=1, keepdims=True)
        weights[g, 0:per_dev, :] = jnp.broadcast_to(count, (per_dev, LEAF // 2))
    side_odd[...] = jnp.zeros_like(side_odd)
    panel_odd[...] = jnp.zeros_like(panel_odd)
    fill_left(0, left_even)
    for half in range(2):
        fill_dist(half, dist_even, left_even, 0)

    steps = 2 * per_dev

    def body(pair, carry):
        g = pair * 2

        @pl.when(g == per_dev)
        def _():
            near_copy(0).wait()
            for copy in oct_copies:
                copy.wait()
            for copy in leaf_copies:
                copy.start()

        @pl.when(g == 2 * per_dev)
        def _():
            near_copy(1).wait()

        for i in range(steps):
            later = (i + 1) % steps
            before = (i - 1) % steps
            before_g = jnp.maximum(g - 1, 0) if i == 0 else g + before // per_dev
            for part in range(8):
                if part == 0 or part == 4:
                    fill_dist(
                        part // 4, dists[later % 2], lefts[later // per_dev], later % per_dev
                    )
                if part == 1 or part == 5:
                    apply(
                        part // 4, before_g, before % per_dev,
                        side_refs[before // per_dev], panels[before % 2],
                    )
                if part == 6 and i == 0:
                    fill_side(g, side_even)
                    fill_left(g + 1, left_odd)
                if part == 6 and i == per_dev:
                    fill_side(g + 1, side_odd)
                    fill_left(g + 2, left_even)
                fill_panel(part, panels[i % 2], dists[i % 2])
        return carry

    lax.fori_loop(0, total // 2, body, 0)
    for half in range(2):
        apply(half, total - 1, per_dev - 1, side_odd, panel_odd)

    for copy in leaf_copies:
        copy.wait()

    dev = me_oct * n_leaf + me
    mine = skel[:, pl.ds(pl.multiple_of(dev * ranks, ranks), ranks)]
    left = features(mine, True).T.astype(BF16)
    far = far_ref[pl.ds(pl.multiple_of(dev * per_dev, per_dev), per_dev), :]
    far_coef = jnp.zeros((ranks, RHS), F32)
    for o in range(n_oct):
        width = n_leaf * ranks
        right = features(skel[:, o * width:(o + 1) * width], False).astype(BF16)
        dist = jnp.dot(left, right, preferred_element_type=F32)
        leaf_id = lax.broadcasted_iota(jnp.int32, (per_dev, width), 1) // RANK + o * n_leaf * per_dev
        count = jnp.zeros((per_dev, width), F32)
        for j in range(FAR):
            count += jnp.where(far[:, j:j + 1] == leaf_id, 1.0, 0.0)
        weight = jnp.concatenate(
            [jnp.broadcast_to(count[a:a + 1, :], (RANK, width)) for a in range(per_dev)], axis=0
        )
        block = coefs[o].reshape(width, RHS)
        far_coef += jnp.dot((matern(dist) * weight).astype(BF16), block, preferred_element_type=F32)
    far_side = far_coef.T.astype(BF16)
    scale = 1.0 / math.sqrt(NEAR * LEAF)
    owner = lax.broadcasted_iota(jnp.int32, (ranks, LEAF), 0) // RANK
    for a in range(per_dev):
        cols = slice(a * LEAF, (a + 1) * LEAF)
        tiled = jnp.concatenate([basis_ref[:, cols].astype(F32)] * per_dev, axis=0)
        block = jnp.where(owner == a, tiled, 0.0).astype(BF16)
        total = acc[:, cols] + jnp.dot(far_side, block, preferred_element_type=F32)
        out_ref[cols, :] = (total * scale).T.astype(BF16)


def local(coords, skeleton, basis, probes, near_list, far_list):
    per_dev = near_list.shape[0]
    n_leaf = lax.axis_size("leaf")
    n_oct = lax.axis_size("oct")
    rows = per_dev * LEAF
    ranks = per_dev * RANK
    leaves = n_oct * n_leaf * per_dev
    skel = jnp.transpose(skeleton, (0, 2, 1)).reshape(3, leaves * RANK)
    vmem = pl.BlockSpec(memory_space=pltpu.VMEM)
    return pl.pallas_call(
        functools.partial(kernel, n_oct, n_leaf, per_dev),
        out_shape=jax.ShapeDtypeStruct((rows, RHS), BF16),
        in_specs=[pl.BlockSpec(memory_space=pltpu.HBM)] * 6,
        out_specs=vmem,
        scratch_shapes=[
            pltpu.VMEM((8, n_leaf * rows), F32),
            pltpu.VMEM((8, leaves * RANK), F32),
            pltpu.VMEM((FEATURES, rows), BF16),
            pltpu.VMEM((RHS, rows), F32),
            pltpu.VMEM((3, rows, RHS), BF16),
            pltpu.VMEM((n_oct, n_leaf, ranks, RHS), BF16),
            pltpu.VMEM((3 * per_dev, 8, LEAF // 2), F32),
            pltpu.VMEM((LEAF, LEAF), F32),
            pltpu.VMEM((LEAF, LEAF), F32),
            pltpu.VMEM((LEAF, LEAF), BF16),
            pltpu.VMEM((LEAF, LEAF), BF16),
            pltpu.VMEM((RHS, LEAF), BF16),
            pltpu.VMEM((RHS, LEAF), BF16),
            pltpu.VMEM((LEAF, FEATURES), BF16),
            pltpu.VMEM((LEAF, FEATURES), BF16),
            pltpu.VMEM(coords.shape, F32),
            pltpu.VMEM(skel.shape, F32),
            pltpu.VMEM(basis.shape, BF16),
            pltpu.VMEM(near_list.shape, jnp.int32),
            pltpu.VMEM(far_list.shape, jnp.int32),
            pltpu.SemaphoreType.DMA((6,)),
            pltpu.SemaphoreType.DMA((2,)),
            pltpu.SemaphoreType.DMA((2,)),
            pltpu.SemaphoreType.DMA((n_oct - 1,)),
            pltpu.SemaphoreType.DMA((n_oct - 1,)),
            pltpu.SemaphoreType.DMA((n_leaf - 1,)),
            pltpu.SemaphoreType.DMA((n_leaf - 1,)),
        ],
        compiler_params=pltpu.CompilerParams(
            collective_id=0, has_side_effects=True, vmem_limit_bytes=60 * 1024 * 1024
        ),
    )(coords, skel, basis, probes, near_list, far_list)


def solution(mesh):
    in_specs = (
        P(None, ("copies", "oct")),
        P(None, None, "copies"),
        P(None, ("copies", "oct", "leaf")),
        P(("copies", "oct", "leaf"), None),
        P(("copies", "oct", "leaf"), None),
        P("copies", None),
    )
    out_specs = P(("copies", "oct", "leaf"), None)
    return jax.shard_map(local, mesh=mesh, in_specs=in_specs, out_specs=out_specs, check_vma=False)
```
